32 devices in a mesh: pod: 2 (over x), d: 16 (over z, y, core).
Axes of the slice: x: 2, y: 2, z: 4, core: 2. Of those that a mesh axis runs over, the one named last changes fastest.
Arguments:
- x: bfloat16 [32, 1024, 2048], P(('pod', 'd')), parts along dimension 0
- prompt_len: int32 [32], P(('pod', 'd')), parts along dimension 0
- ln_scale: float32 [2048], P('d')
- w_in: bfloat16 [2048, 18944], P('d')
- w_out: bfloat16 [10240, 2048], P(None, 'd')
Outputs:
- output 1: bfloat16 [32, 1024, 2048], P(('pod', 'd')), parts along dimension 0
- output 2: bfloat16 [32, 1024, 256], P(('pod', 'd')), parts along dimension 0
- output 3: bfloat16 [32, 1024, 256], P(('pod', 'd')), parts along dimension 0
There are 2 independent parts. The reference program is written for one: setup_inputs(seed, part) draws one part's arguments, and reference() takes and returns one part's arrays. A program takes and returns all parts, laid end to end along the dimension named above; an argument that names none is the same for every part.
All inputs are finite; a program needn't handle non-finite values.
Results may differ from the reference program's by a relative error of at most 0.00441177.
Values are sent between devices in bfloat16 or wider.
A program may use at most 1 GiB of HBM per device.

```python
import math
import jax
import jax.numpy as jnp
from jax import lax

E = 2048
F = 8192
HEADS = 8
HEAD = 256
T = 1024
BATCH = 16

COLS_IN = 2 * F + HEADS * HEAD + 2 * HEAD
ROWS_OUT = F + HEADS * HEAD
EPS = 1e-6
ROPE_BASE = 10000.0


def setup_inputs(seed: int = 0, part: int = 0) -> dict:
    shared_key = jax.random.key(seed)
    part_key = jax.random.fold_in(jax.random.key(seed + 1), part)
    key_x, key_len, key_full = jax.random.split(part_key, 3)
    key_ln, key_in, key_out = jax.random.split(shared_key, 3)
    x = jax.random.normal(key_x, (BATCH, T, E), jnp.float32).astype(jnp.bfloat16)
    drawn_len = jax.random.randint(key_len, (BATCH,), 1, T + 1, dtype=jnp.int32)
    full_slot = jax.random.randint(key_full, (), 0, BATCH, dtype=jnp.int32)
    prompt_len = jnp.where(jnp.arange(BATCH) == full_slot, T, drawn_len).astype(jnp.int32)
    ln_scale = 1.0 + 0.25 * jax.random.normal(key_ln, (E,), jnp.float32)
    q_gain = math.sqrt(0.5 * math.log(T))
    col_gain = jnp.concatenate([
        jnp.ones((2 * F,), jnp.float32),
        jnp.full((HEADS * HEAD,), q_gain, jnp.float32),
        jnp.ones((2 * HEAD,), jnp.float32)])
    w_in = (jax.random.normal(key_in, (E, COLS_IN), jnp.float32) * (E ** -0.5) * col_gain).astype(jnp.bfloat16)
    row_gain = jnp.concatenate([
        jnp.full((F,), F ** -0.5, jnp.float32),
        jnp.full((HEADS * HEAD,), (HEADS * HEAD) ** -0.5, jnp.float32)])
    w_out = (jax.random.normal(key_out, (ROWS_OUT, E), jnp.float32) * row_gain[:, None]).astype(jnp.bfloat16)
    return {"x": x, "prompt_len": prompt_len, "ln_scale": ln_scale, "w_in": w_in, "w_out": w_out}


def rope_tables():
    half_dim = HEAD // 2
    inv_freq = ROPE_BASE ** (-2.0 * jnp.arange(half_dim, dtype=jnp.float32) / HEAD)
    angles = jnp.arange(T, dtype=jnp.float32)[:, None] * inv_freq[None, :]
    return jnp.cos(angles), jnp.sin(angles)


def apply_rope(rope_in, cos_b, sin_b):
    half_dim = rope_in.shape[-1] // 2
    lower_half = rope_in[..., :half_dim]
    upper_half = rope_in[..., half_dim:]
    return jnp.concatenate([lower_half * cos_b - upper_half * sin_b, upper_half * cos_b + lower_half * sin_b], axis=-1)


def reference(x, prompt_len, ln_scale, w_in, w_out):
    cos_t, sin_t = rope_tables()
    positions = jnp.arange(T)
    causal = positions[None, :] <= positions[:, None]
    q_start = 2 * F
    k_start = q_start + HEADS * HEAD
    v_start = k_start + HEAD

    def one_sequence(seq_args):
        x_seq, seq_len = seq_args
        x_float = x_seq.astype(jnp.float32)
        centered = x_float - jnp.mean(x_float, axis=-1, keepdims=True)
        var_val = jnp.mean(centered * centered, axis=-1, keepdims=True)
        h_norm = (centered * lax.rsqrt(var_val + EPS) * ln_scale).astype(jnp.bfloat16)
        projected = jnp.dot(h_norm, w_in, preferred_element_type=jnp.float32)
        gated = (jax.nn.silu(projected[:, :F]) * projected[:, F:q_start]).astype(jnp.bfloat16)
        q_rot = apply_rope(projected[:, q_start:k_start].reshape(T, HEADS, HEAD), cos_t[:, None, :], sin_t[:, None, :]).astype(jnp.bfloat16)
        k_rot = apply_rope(projected[:, k_start:v_start], cos_t, sin_t).astype(jnp.bfloat16)
        v_val = projected[:, v_start:].astype(jnp.bfloat16)
        scores = jnp.einsum("thd,sd->hts", q_rot.astype(jnp.float32), k_rot.astype(jnp.float32)) * (1.0 / math.sqrt(HEAD))
        allowed = causal & (positions[None, :] < seq_len)
        probs_bf = jax.nn.softmax(jnp.where(allowed[None, :, :], scores, -1e30), axis=-1).astype(jnp.bfloat16)
        attn_out = jnp.einsum("hts,sd->thd", probs_bf.astype(jnp.float32), v_val.astype(jnp.float32)).astype(jnp.bfloat16).reshape(T, HEADS * HEAD)
        mixed_rows = jnp.concatenate([gated, attn_out], axis=-1)
        out_sum = jnp.dot(mixed_rows, w_out, preferred_element_type=jnp.float32)
        return (x_float + out_sum).astype(jnp.bfloat16), k_rot, v_val

    y_out, k_cache, v_cache = lax.map(one_sequence, (x, prompt_len))
    return y_out, k_cache, v_cache
```

```python
import functools
import math

import jax
import jax.numpy as jnp
import numpy as np
from jax import lax
from jax.experimental import pallas as pl
from jax.experimental.pallas import tpu as pltpu
from jax.sharding import PartitionSpec as P

MESH = pl.DeviceIdType.MESH
EPS = 1e-6
ROPE_BASE = 10000.0
E, F, HEADS, HEAD, T = 2048, 8192, 8, 256, 1024
Q0, K0 = 2 * F, 2 * F + HEADS * HEAD
UNIT = 512
TRIPLES = 19
NU = 3 * TRIPLES
M = 18
R = NU - M
LAG = 1
XLAG = 4
OFF = 4 * LAG + XLAG + 1
STEPS = 2 * TRIPLES + OFF + 1
RB = 256


def unit_of(s, pod):
    m, b = s // 2, s % 2
    return jnp.where(s < 2 * M, 3 * m + (1 - b) * pod + 2 * b, 3 * M + (s - 2 * M))


def device_of(r, c):
    y = r // 4
    z = (1 - y) * r + y * (7 - r)
    return (z * 2 + y) * 2 + c


def layer_kernel(x, plen, ln, w_in, w_out, cos, sin, y_out, k_out, v_out, G,
                 Pv, xv, h, acc, wg, wp, wx, wo, woa, a, q, kk, vv, o, cs, sn, ln_all,
                 pack_sem, own_sem, in_sem, out_sem, ld, rs, rr, xs, xr, ds_, dr, ls, lr):
    pod, d = lax.axis_index("pod"), lax.axis_index("d")
    c, yy, zz = d % 2, (d // 2) % 2, d // 4
    r = (1 - yy) * zz + yy * (7 - zz)
    right, left, partner = device_of((r + 1) % 8, c), device_of((r + 7) % 8, c), device_of(r, 1 - c)

    def pack_in(u, col):
        for j in range(4):
            pltpu.make_async_copy(w_in.at[:, pl.ds(pl.multiple_of(col + 128 * j, 128), 128)],
                                  Pv.at[u, pl.ds(128 * j, 128), :], pack_sem).start()

    def pack_out(u, row):
        pltpu.make_async_copy(w_out.at[pl.ds(row, UNIT), :], Pv.at[u], pack_sem).start()

    for u, col in ((0, K0), (1, Q0), (2, Q0 + 512), (3, Q0 + 1024), (4, Q0 + 1536)):
        pack_in(u, col)
    for i in range(4):
        pack_out(5 + i, F + UNIT * i)

    def pack_mlp(j, _):
        pack_in(9 + 3 * j, UNIT * j)
        pack_in(10 + 3 * j, F + UNIT * j)
        pack_out(11 + 3 * j, UNIT * j)
        return 0

    lax.fori_loop(0, TRIPLES - 3, pack_mlp, 0)
    x_in = pltpu.make_async_copy(x, xv, in_sem.at[0])
    cos_in = pltpu.make_async_copy(cos, cs, in_sem.at[1])
    sin_in = pltpu.make_async_copy(sin, sn, in_sem.at[2])
    x_in.start()
    cos_in.start()
    sin_in.start()

    bar = pltpu.get_barrier_semaphore()
    for t in range(1, 16):
        pl.semaphore_signal(bar, inc=1, device_id=(pod, (d + t) % 16), device_id_type=MESH)
    pl.semaphore_signal(bar, inc=1, device_id=(1 - pod, d), device_id_type=MESH)
    pltpu.make_async_copy(Pv, Pv, pack_sem).wait()
    own = pltpu.make_async_copy(Pv, G.at[:, c, 0], own_sem)
    own.start()
    pl.semaphore_wait(bar, 16)

    def ring(src, dst, s, e, to):
        return pltpu.make_async_remote_copy(src_ref=src, dst_ref=dst, send_sem=rs.at[s, e], recv_sem=rr.at[s, e],
                                            device_id=(pod, to), device_id_type=MESH)

    half0, half1 = pl.ds(0, 256), pl.ds(256, 256)

    def cw(s, hop):
        u = unit_of(s, pod)
        if hop == 1:
            return ring(Pv.at[u], G.at[u, c, 7], s, 0, right)
        if hop == 4:
            return ring(G.at[u, c, 5, half0], G.at[u, c, 4, half0], s, 6, right)
        return ring(G.at[u, c, 9 - hop], G.at[u, c, 8 - hop], s, 2 * (hop - 1), right)

    def ccw(s, hop):
        u = unit_of(s, pod)
        if hop == 1:
            return ring(Pv.at[u], G.at[u, c, 1], s, 1, left)
        if hop == 4:
            return ring(G.at[u, c, 3, half1], G.at[u, c, 4, half1], s, 7, left)
        return ring(G.at[u, c, hop - 1], G.at[u, c, hop], s, 2 * hop - 1, left)

    def cross(m, u):
        return pltpu.make_async_remote_copy(src_ref=G.at[u, c, pl.ds(1, 7)], dst_ref=G.at[u, c, pl.ds(1, 7)],
                                            send_sem=xs.at[m], recv_sem=xr.at[m],
                                            device_id=(1 - pod, d), device_id_type=MESH)

    def share(u, core):
        return pltpu.make_async_remote_copy(src_ref=G.at[u, core], dst_ref=G.at[u, core],
                                            send_sem=ds_.at[u], recv_sem=dr.at[u],
                                            device_id=(pod, partner), device_id_type=MESH)

    def ln_copy(t):
        return pltpu.make_async_remote_copy(src_ref=ln, dst_ref=ln_all.at[d], send_sem=ls.at[t], recv_sem=lr.at[t],
                                            device_id=(pod, (d + t) % 16), device_id_type=MESH)

    for t in range(1, 16):
        ln_copy(t).start()
    ln_all[pl.ds(d, 1)] = ln[...][None]

    def load_in(u, dst, sem):
        for j in range(4):
            pltpu.make_async_copy(G.at[u, :, :, pl.ds(128 * j, 128), :], dst.at[:, :, :, pl.ds(128 * j, 128)], sem).start()

    def load_out(u, dst, sem):
        for cc in range(2):
            for rel in range(8):
                src = device_of((r + rel) % 8, cc)
                pltpu.make_async_copy(G.at[u, cc, rel], dst.at[:, pl.ds(pl.multiple_of(src * 128, 128), 128)], sem).start()

    def wait_load(dst, sem):
        pltpu.make_async_copy(dst, dst, sem).wait()

    def rows(b):
        return pl.ds(b * RB, RB)

    def norm(b):
        xf = xv[rows(b), :].astype(jnp.float32)
        xc = xf - jnp.mean(xf, axis=-1, keepdims=True)
        xn = xc * lax.rsqrt(jnp.mean(xc * xc, axis=-1, keepdims=True) + EPS)
        for src in range(16):
            sc, sy, sz = src % 2, (src // 2) % 2, src // 4
            sr = (1 - sy) * sz + sy * (7 - sz)
            at = sc * 8 + (sr - r + 8) % 8
            h[rows(b), pl.ds(pl.multiple_of(at * 128, 128), 128)] = (
                xn[:, src * 128:(src + 1) * 128] * ln_all[src]).astype(jnp.bfloat16)
        acc[rows(b), :] = jnp.zeros((RB, E), jnp.float32)

    def proj(b, w):
        return jnp.dot(h[rows(b), :], w.reshape(E, UNIT), preferred_element_type=jnp.float32)

    def rope(b, u):
        lo, hi = u[:, :128], u[:, 128:]
        cb, sb = cs[rows(b), :], sn[rows(b), :]
        return jnp.concatenate([lo * cb - hi * sb, hi * cb + lo * sb], axis=-1).astype(jnp.bfloat16)

    def proj_kv(b, w):
        u = proj(b, w)
        kk[rows(b), :] = rope(b, u[:, :256])
        vv[rows(b), :] = u[:, 256:].astype(jnp.bfloat16)

    def proj_q(b, w, head):
        u = proj(b, w)
        q[head, rows(b), :] = rope(b, u[:, :256])
        q[head + 1, rows(b), :] = rope(b, u[:, 256:])

    def attend(b, head0):
        n = (b + 1) * RB
        qpos = b * RB + lax.broadcasted_iota(jnp.int32, (RB, n), 0)
        kpos = lax.broadcasted_iota(jnp.int32, (RB, n), 1)
        allowed = (kpos <= qpos) & (kpos < plen[0])

        def one(i, _):
            head = head0 + i
            s = lax.dot_general(q[head, rows(b), :], kk[0:n, :], (((1,), (1,)), ((), ())),
                                preferred_element_type=jnp.float32) * (1.0 / math.sqrt(HEAD))
            s = jnp.where(allowed, s, -1e30)
            e = jnp.exp(s - jnp.max(s, axis=-1, keepdims=True))
            p = (e * (1.0 / jnp.sum(e, axis=-1, keepdims=True))).astype(jnp.bfloat16)
            o[rows(b), pl.ds(pl.multiple_of(head * HEAD, HEAD), HEAD)] = jnp.dot(
                p, vv[0:n, :], preferred_element_type=jnp.float32).astype(jnp.bfloat16)
            return 0

        lax.fori_loop(0, 4, one, 0)

    def mlp_in(b, slot):
        g = proj(b, wg[slot])
        p = proj(b, wp[slot])
        a[rows(b), :] = (g * jax.nn.sigmoid(g) * p).astype(jnp.bfloat16)

    def y_copy(b):
        return pltpu.make_async_copy(xv.at[rows(b), :], y_out.at[rows(b), :], out_sem.at[b])

    k_copy = pltpu.make_async_copy(kk, k_out, out_sem.at[4])
    v_copy = pltpu.make_async_copy(vv, v_out, out_sem.at[5])

    def slice_in(b, t, slot):
        @pl.when(t == 0)
        def _():
            if b == 0:
                wait_load(wg.at[0], ld.at[0, 0])
                wait_load(wp.at[0], ld.at[0, 1])
            proj_kv(b, wg[0])
            proj_q(b, wp[0], 0)

        @pl.when(t == 1)
        def _():
            if b == 0:
                wait_load(wg.at[1], ld.at[1, 0])
            proj_q(b, wg[1], 4)

        @pl.when(t == 2)
        def _():
            if b == 0:
                k_copy.start()
                v_copy.start()
            attend(b, 0)

        @pl.when((t >= 3) & (t < TRIPLES))
        def _():
            if b == 0:
                wait_load(wg.at[slot], ld.at[slot, 0])
                wait_load(wp.at[slot], ld.at[slot, 1])
            mlp_in(b, slot)

        @pl.when((t >= 3) & (t < 7))
        def _():
            if b == 0:
                wait_load(woa, ld.at[0, 3])
            acc[rows(b), :] += jnp.dot(o[rows(b), pl.ds(pl.multiple_of((t - 3) * UNIT, UNIT), UNIT)], woa[...],
                                       preferred_element_type=jnp.float32)

    def slice_out(b, t, slot):
        @pl.when(t == 0)
        def _():
            if b == 0:
                wait_load(wx, ld.at[1, 3])
            proj_q(b, wx[...], 2)

        @pl.when(t == 1)
        def _():
            if b == 0:
                wait_load(wp.at[1], ld.at[1, 1])
            proj_q(b, wp[1], 6)

        @pl.when(t == 2)
        def _():
            attend(b, 4)

        @pl.when((t >= 3) & (t < TRIPLES))
        def _():
            if b == 0:
                wait_load(wo.at[slot], ld.at[slot, 2])
            acc[rows(b), :] += jnp.dot(a[rows(b), :], wo[slot], preferred_element_type=jnp.float32)

        @pl.when(t == TRIPLES - 1)
        def _():
            xv[rows(b), :] = (xv[rows(b), :].astype(jnp.float32) + acc[rows(b), :]).astype(jnp.bfloat16)
            if b:
                y_copy(b - 1).start()

    def arrive(t):
        @pl.when((t >= 0) & (t < TRIPLES))
        def _():
            for i in range(3):
                share(3 * t + i, 1 - c).wait_recv()
            slot = t % 2

            @pl.when(t == 0)
            def _():
                load_in(0, wg.at[0], ld.at[0, 0])
                load_in(1, wp.at[0], ld.at[0, 1])
                load_in(2, wx, ld.at[1, 3])

            @pl.when(t == 1)
            def _():
                load_in(3, wg.at[1], ld.at[1, 0])
                load_in(4, wp.at[1], ld.at[1, 1])

            @pl.when(t >= 3)
            def _():
                load_in(3 * t, wg.at[slot], ld.at[slot, 0])
                load_in(3 * t + 1, wp.at[slot], ld.at[slot, 1])
                load_out(3 * t + 2, wo.at[slot], ld.at[slot, 2])

            @pl.when((t >= 3) & (t < 7))
            def _():
                load_out(t + 2, woa, ld.at[0, 3])

    own.wait()

    def step(i, odd):
        is_out = odd == OFF % 2
        t = (i - OFF) // 2 - 1 if is_out else (i - OFF - 1) // 2
        t = jnp.where(i < OFF, -1, t)

        def work(b):
            (slice_out if is_out else slice_in)(b, t, t % 2)
            if not is_out:
                @pl.when(i == (2 if OFF % 2 else 3))
                def _():
                    if b == 0:
                        x_in.wait()
                        for j in range(1, 16):
                            ln_copy(j).wait_recv()
                        cos_in.wait()
                        sin_in.wait()
                    norm(b)

        @pl.when(i < R)
        def _():
            cw(i, 1).start()
            ccw(i, 1).start()

        for hop in (2, 3, 4):
            s = i - LAG * (hop - 1)

            @pl.when((s >= 0) & (s < R))
            def _():
                cw(s, hop - 1).wait_recv()
                cw(s, hop).start()
                ccw(s, hop - 1).wait_recv()
                ccw(s, hop).start()

            work(hop - 2)

        s = i - LAG * 4

        @pl.when((s >= 0) & (s < R))
        def _():
            cw(s, 4).wait_recv()
            ccw(s, 4).wait_recv()
            u = unit_of(s, pod)

            @pl.when((s < 2 * M) & (s % 2 == 0))
            def _():
                cross(s // 2, u).start()

            share(u, c).start()

        s = i - LAG * 4 - XLAG

        @pl.when((s >= 0) & (s < 2 * M) & (s % 2 == 0))
        def _():
            u = 3 * (s // 2) + 1 - pod
            cross(s // 2, u).wait_recv()
            share(u, c).start()

        work(3)
        if is_out:
            arrive(jnp.where(i < OFF, -1, (i - OFF) // 2))

    def two_steps(it, _):
        step(2 * it, 0)
        step(2 * it + 1, 1)
        return 0

    lax.fori_loop(0, (STEPS + 1) // 2, two_steps, 0)

    y_copy(3).start()
    for b in range(4):
        y_copy(b).wait()
    k_copy.wait()
    v_copy.wait()
    for t in range(1, 16):
        ln_copy(t).wait_send()

    def sent_units(u, _):
        share(u, c).wait_send()
        return 0

    def sent_ring(s, _):
        for hop in (1, 2, 3, 4):
            cw(s, hop).wait_send()
            ccw(s, hop).wait_send()
        return 0

    def sent_cross(m, _):
        cross(m, 3 * m + pod).wait_send()
        return 0

    lax.fori_loop(0, NU, sent_units, 0)
    lax.fori_loop(0, R, sent_ring, 0)
    lax.fori_loop(0, M, sent_cross, 0)


def layer(x, plen, ln, w_in, w_out, cos, sin):
    bf, f32 = jnp.bfloat16, jnp.float32
    anyspace = pl.BlockSpec(memory_space=pl.ANY)
    vmem = pltpu.VMEM
    dma = pltpu.SemaphoreType.DMA
    return pl.pallas_call(
        layer_kernel,
        name="layer",
        out_shape=(jax.ShapeDtypeStruct((T, E), bf), jax.ShapeDtypeStruct((T, HEAD), bf),
                   jax.ShapeDtypeStruct((T, HEAD), bf), jax.ShapeDtypeStruct((NU, 2, 8, UNIT, 128), bf)),
        in_specs=[anyspace, pl.BlockSpec(memory_space=pltpu.SMEM), pl.BlockSpec(memory_space=vmem),
                  anyspace, anyspace, anyspace, anyspace],
        out_specs=(anyspace,) * 4,
        scratch_shapes=[
            vmem((NU, UNIT, 128), bf), vmem((T, E), bf), vmem((T, E), bf), vmem((T, E), f32),
            vmem((2, 2, 8, 128, UNIT), bf), vmem((2, 2, 8, 128, UNIT), bf), vmem((2, 8, 128, UNIT), bf),
            vmem((2, UNIT, E), bf), vmem((UNIT, E), bf), vmem((T, UNIT), bf),
            vmem((HEADS, T, HEAD), bf), vmem((T, HEAD), bf), vmem((T, HEAD), bf), vmem((T, HEADS * HEAD), bf),
            vmem((T, 128), f32), vmem((T, 128), f32), vmem((16, 1, 128), f32),
            dma, dma, dma((3,)), dma((6,)), dma((2, 4)), dma((R, 8)), dma((R, 8)), dma((M,)), dma((M,)),
            dma((NU,)), dma((NU,)), dma((16,)), dma((16,))],
        compiler_params=pltpu.CompilerParams(collective_id=0, has_side_effects=True,
                                             vmem_limit_bytes=63 * 1024 * 1024),
    )(x, plen, ln, w_in, w_out, cos, sin)


def rope_tables():
    inv_freq = (ROPE_BASE ** (-2.0 * np.arange(HEAD // 2, dtype=np.float32) / HEAD)).astype(np.float32)
    angles = np.arange(T, dtype=np.float32)[:, None] * inv_freq[None, :]
    return np.cos(angles).astype(np.float32), np.sin(angles).astype(np.float32)


def solution(mesh):
    batch = P(("pod", "d"))
    cos, sin = rope_tables()

    def local_layer(x, plen, ln, w_in, w_out):
        y, k, v, _ = layer(x[0], plen, ln[None], w_in, w_out, cos, sin)
        return y[None], k[None], v[None]

    return jax.shard_map(local_layer, mesh=mesh,
                         in_specs=(batch, batch, P("d"), P("d", None), P(None, "d")),
                         out_specs=(batch, batch, batch), check_vma=False)
```

```python
import functools
import math

import jax
import jax.numpy as jnp
import numpy as np
from jax import lax
from jax.experimental import pallas as pl
from jax.experimental.pallas import tpu as pltpu
from jax.sharding import PartitionSpec as P

MESH = pl.DeviceIdType.MESH
EPS = 1e-6
ROPE_BASE = 10000.0
E, F, HEADS, HEAD, T = 2048, 8192, 8, 256, 1024
Q0, K0 = 2 * F, 2 * F + HEADS * HEAD
UNIT = 512
TRIPLES = 19
NU = 3 * TRIPLES
LAST = TRIPLES - 1
M = 18
R = NU - M
LAG = 1
XLAG = 1
OFF = 4 * LAG + XLAG + 1
STEPS = 2 * LAST + OFF + 2
DONE = 8
RB = 256


def unit_of(s, pod):
    m, b = s // 2, s % 2
    return jnp.where(s < 2 * M, 3 * m + (1 - b) * pod + 2 * b, 3 * M + (s - 2 * M))


def device_of(r, c):
    y = r // 4
    z = (1 - y) * r + y * (7 - r)
    return (z * 2 + y) * 2 + c


def layer_kernel(x, plen, ln, w_in, w_out, tab, y_out, k_out, v_out, G,
                 Pv, xv, h, acc, wg, wp, wx, wo, woa, a, q, kk, vv, o, cs, sn, tb, ln_all,
                 pack_sem, own_sem, in_sem, out_sem, ld, rs, rr, xs, xr, ds_, dr, ls, lr):
    pod, d = lax.axis_index("pod"), lax.axis_index("d")
    c, yy, zz = d % 2, (d // 2) % 2, d // 4
    r = (1 - yy) * zz + yy * (7 - zz)
    right, left, partner = device_of((r + 1) % 8, c), device_of((r + 7) % 8, c), device_of(r, 1 - c)

    def pack_in(u, col, first=1):
        for j in range(4):
            pltpu.make_async_copy(w_in.at[:, pl.ds(pl.multiple_of(col + 128 * j, 128), 128)],
                                  Pv.at[u, pl.ds(128 * j, 128), :], pack_sem.at[first]).start()

    def pack_out(u, row):
        pltpu.make_async_copy(w_out.at[pl.ds(row, UNIT), :], Pv.at[u], pack_sem.at[1]).start()

    for u, col in ((0, K0), (1, Q0), (2, Q0 + 512)):
        pack_in(u, col, 0)
    bar = pltpu.get_barrier_semaphore()
    for t in range(1, 16):
        pl.semaphore_signal(bar, inc=1, device_id=(pod, (d + t) % 16), device_id_type=MESH)
    pl.semaphore_signal(bar, inc=1, device_id=(1 - pod, d), device_id_type=MESH)
    x_in = pltpu.make_async_copy(x, xv, in_sem.at[0])
    tab_in = pltpu.make_async_copy(tab, tb, in_sem.at[1])
    own = pltpu.make_async_copy(Pv, G.at[:, c, 0], own_sem)
    pltpu.make_async_copy(Pv.at[pl.ds(0, 3)], Pv.at[pl.ds(0, 3)], pack_sem.at[0]).wait()
    pl.semaphore_wait(bar, 16)

    def ring(src, dst, s, e, to):
        return pltpu.make_async_remote_copy(src_ref=src, dst_ref=dst, send_sem=rs.at[s, e], recv_sem=rr.at[s, e],
                                            device_id=(pod, to), device_id_type=MESH)

    half0, half1 = pl.ds(0, 256), pl.ds(256, 256)

    def cw(s, hop):
        u = unit_of(s, pod)
        if hop == 1:
            return ring(Pv.at[u], G.at[u, c, 7], s, 0, right)
        if hop == 4:
            return ring(G.at[u, c, 5, half0], G.at[u, c, 4, half0], s, 6, right)
        return ring(G.at[u, c, 9 - hop], G.at[u, c, 8 - hop], s, 2 * (hop - 1), right)

    def ccw(s, hop):
        u = unit_of(s, pod)
        if hop == 1:
            return ring(Pv.at[u], G.at[u, c, 1], s, 1, left)
        if hop == 4:
            return ring(G.at[u, c, 3, half1], G.at[u, c, 4, half1], s, 7, left)
        return ring(G.at[u, c, hop - 1], G.at[u, c, hop], s, 2 * hop - 1, left)

    def cross(m, u, at, n):
        return pltpu.make_async_remote_copy(src_ref=G.at[u, c, pl.ds(at, n)], dst_ref=G.at[u, c, pl.ds(at, n)],
                                            send_sem=xs.at[m], recv_sem=xr.at[m],
                                            device_id=(1 - pod, d), device_id_type=MESH)

    def share(u, core, at=0, n=8, src=None):
        here = G.at[u, core, pl.ds(at, n)]
        return pltpu.make_async_remote_copy(src_ref=here if src is None else src, dst_ref=here,
                                            send_sem=ds_.at[u], recv_sem=dr.at[u],
                                            device_id=(pod, partner), device_id_type=MESH)

    def pass_on(s, at):
        u = unit_of(s, pod)

        @pl.when((s < 2 * M) & (s % 2 == 0))
        def _():
            cross(s // 2, u, at, 1).start()

        share(u, c, at, 1).start()

    def ln_copy(t):
        return pltpu.make_async_remote_copy(src_ref=ln, dst_ref=ln_all.at[d], send_sem=ls.at[t], recv_sem=lr.at[t],
                                            device_id=(pod, (d + t) % 16), device_id_type=MESH)

    def send_own(s):
        cw(s, 1).start()
        ccw(s, 1).start()
        u = unit_of(s, pod)
        share(u, c, 0, 1, Pv.at[pl.ds(u, 1)]).start()

    send_own(0)
    for t in range(1, 16):
        ln_copy(t).start()
    ln_all[pl.ds(d, 1)] = ln[...][None]
    x_in.start()
    tab_in.start()
    for u, col in ((3, Q0 + 1024), (4, Q0 + 1536)):
        pack_in(u, col)
    pack_out(5, F)
    for i in range(3):
        pack_out(3 * LAST + i, F + UNIT * (i + 1))

    def pack_mlp(j, _):
        pack_in(6 + 3 * j, UNIT * j)
        pack_in(7 + 3 * j, F + UNIT * j)
        pack_out(8 + 3 * j, UNIT * j)
        return 0

    lax.fori_loop(0, F // UNIT, pack_mlp, 0)

    def load_in(u, dst, sem):
        for j in range(4):
            pltpu.make_async_copy(G.at[u, :, :, pl.ds(128 * j, 128), :], dst.at[:, :, :, pl.ds(128 * j, 128)], sem).start()

    def load_out(u, dst, sem):
        for cc in range(2):
            for rel in range(8):
                src = device_of((r + rel) % 8, cc)
                pltpu.make_async_copy(G.at[u, cc, rel], dst.at[:, pl.ds(pl.multiple_of(src * 128, 128), 128)], sem).start()

    def wait_load(dst, sem):
        pltpu.make_async_copy(dst, dst, sem).wait()

    def rows(b):
        return pl.ds(b * RB, RB)

    def norm(b):
        xf = xv[rows(b), :].astype(jnp.float32)
        xc = xf - jnp.mean(xf, axis=-1, keepdims=True)
        xn = xc * lax.rsqrt(jnp.mean(xc * xc, axis=-1, keepdims=True) + EPS)
        for src in range(16):
            sc, sy, sz = src % 2, (src // 2) % 2, src // 4
            sr = (1 - sy) * sz + sy * (7 - sz)
            at = sc * 8 + (sr - r + 8) % 8
            h[rows(b), pl.ds(pl.multiple_of(at * 128, 128), 128)] = (
                xn[:, src * 128:(src + 1) * 128] * ln_all[src]).astype(jnp.bfloat16)
        acc[rows(b), :] = xf

    def tables(b):
        cb, sb = tb[2], tb[3]
        for i in range(RB // 32):
            n = b * (RB // 32) + i
            ca, sa = tb[0, n:n + 1, :], tb[1, n:n + 1, :]
            cs[pl.ds(32 * n, 32), :] = ca * cb - sa * sb
            sn[pl.ds(32 * n, 32), :] = sa * cb + ca * sb

    def proj(b, w):
        return jnp.dot(h[rows(b), :], w.reshape(E, UNIT), preferred_element_type=jnp.float32)

    def rope(b, u):
        lo, hi = u[:, :128], u[:, 128:]
        cb, sb = cs[rows(b), :], sn[rows(b), :]
        return jnp.concatenate([lo * cb - hi * sb, hi * cb + lo * sb], axis=-1).astype(jnp.bfloat16)

    def proj_kv(b, w):
        u = proj(b, w)
        kk[rows(b), :] = rope(b, u[:, :256])
        vv[rows(b), :] = u[:, 256:].astype(jnp.bfloat16)

    def proj_q(b, w, head):
        u = proj(b, w)
        q[head, rows(b), :] = rope(b, u[:, :256])
        q[head + 1, rows(b), :] = rope(b, u[:, 256:])

    def attend(b, head):
        n = (b + 1) * RB
        qpos = b * RB + lax.broadcasted_iota(jnp.int32, (RB, n), 0)
        kpos = lax.broadcasted_iota(jnp.int32, (RB, n), 1)
        allowed = (kpos <= qpos) & (kpos < plen[0])

        s = lax.dot_general(q[head, rows(b), :], kk[0:n, :], (((1,), (1,)), ((), ())),
                            preferred_element_type=jnp.float32) * (1.0 / math.sqrt(HEAD))
        s = jnp.where(allowed, s, -1e30)
        e = jnp.exp(s - jnp.max(s, axis=-1, keepdims=True))
        p = (e * (1.0 / jnp.sum(e, axis=-1, keepdims=True))).astype(jnp.bfloat16)
        o[rows(b), pl.ds(pl.multiple_of(head * HEAD, HEAD), HEAD)] = jnp.dot(
            p, vv[0:n, :], preferred_element_type=jnp.float32).astype(jnp.bfloat16)

    def mlp_in(b, slot):
        g = proj(b, wg[slot])
        p = proj(b, wp[slot])
        a[rows(b), :] = (g * jax.nn.sigmoid(g) * p).astype(jnp.bfloat16)

    def y_copy(b):
        return pltpu.make_async_copy(xv.at[rows(b), :], y_out.at[rows(b), :], out_sem.at[b])

    k_copy = pltpu.make_async_copy(kk, k_out, out_sem.at[4])
    v_copy = pltpu.make_async_copy(vv, v_out, out_sem.at[5])

    def slice_in(b, t, slot):
        @pl.when(t == 0)
        def _():
            if b == 0:
                wait_load(wg.at[0], ld.at[0, 0])
                wait_load(wp.at[0], ld.at[0, 1])
            proj_kv(b, wg[0])
            proj_q(b, wp[0], 0)

        @pl.when(t == 1)
        def _():
            if b == 0:
                wait_load(wg.at[1], ld.at[1, 0])
            proj_q(b, wg[1], 4)

        @pl.when((t >= 2) & (t < LAST))
        def _():
            if b == 0:
                wait_load(wg.at[slot], ld.at[slot, 0])
                wait_load(wp.at[slot], ld.at[slot, 1])
            mlp_in(b, slot)

    def slice_out(b, t, slot):
        @pl.when(t == 0)
        def _():
            if b == 0:
                wait_load(wx, ld.at[1, 3])
            proj_q(b, wx[...], 2)

        @pl.when(t == 1)
        def _():
            if b == 0:
                wait_load(wp.at[1], ld.at[1, 1])
            proj_q(b, wp[1], 6)

        @pl.when((t >= 2) & (t < LAST))
        def _():
            if b == 0:
                wait_load(wo.at[slot], ld.at[slot, 2])
            acc[rows(b), :] += jnp.dot(a[rows(b), :], wo[slot], preferred_element_type=jnp.float32)

    def out_attention(b, i, w):
        return acc[rows(b), :] + jnp.dot(o[rows(b), i * UNIT:(i + 1) * UNIT], w[...], preferred_element_type=jnp.float32)

    def attention(blocks, t, second):
        @pl.when((t >= 2) & (t < 2 + HEADS // 2))
        def _():
            for b in blocks:
                attend(b, 2 * (t - 2) + second)

    def here(u):
        share(u, 1 - c).wait_recv()

    def arrive(t):
        slot = t % 2

        @pl.when((t >= 0) & (t < LAST))
        def _():
            for i in range(3):
                here(3 * t + i)

        @pl.when(t == 0)
        def _():
            load_in(0, wg.at[0], ld.at[0, 0])
            load_in(1, wp.at[0], ld.at[0, 1])
            load_in(2, wx, ld.at[1, 3])

        @pl.when(t == 1)
        def _():
            load_in(3, wg.at[1], ld.at[1, 0])
            load_in(4, wp.at[1], ld.at[1, 1])

        @pl.when((t >= 2) & (t < LAST))
        def _():
            load_in(3 * t, wg.at[slot], ld.at[slot, 0])
            load_in(3 * t + 1, wp.at[slot], ld.at[slot, 1])
            load_out(3 * t + 2, wo.at[slot], ld.at[slot, 2])

        @pl.when(t == 6)
        def _():
            load_out(5, woa, ld.at[0, 3])

        @pl.when(t == LAST)
        def _():
            here(3 * LAST + 1)
            load_out(3 * LAST + 1, wo.at[LAST % 2], ld.at[LAST % 2, 2])

    def step(i, odd):
        is_out = odd == OFF % 2
        t = jnp.where(i < OFF, -1, (i - OFF) // 2)
        slot = t % 2

        def work(n):
            if is_out:
                before = jnp.where(i < OFF, -1, t - 1)
                if n < 2:
                    slice_out(2 * n, before, (t + 1) % 2)
                    slice_out(2 * n + 1, before, (t + 1) % 2)
                    if n == 1:
                        arrive(t)
                elif n == 2:
                    attention((0, 1, 2), t, 0)

                    @pl.when(t == LAST)
                    def _():
                        wait_load(woa, ld.at[0, 3])
                        for b in range(4):
                            acc[rows(b), :] = out_attention(b, 1, woa)
                else:
                    slice_in(0, t, slot)
                    attention((3,), t, 0)
                return
            if n == 0:
                @pl.when(i == (2 if OFF % 2 else 3))
                def _():
                    x_in.wait()
                    for j in range(1, 16):
                        ln_copy(j).wait_recv()
                    tab_in.wait()

                @pl.when(t == 2)
                def _():
                    k_copy.start()
                    v_copy.start()

            @pl.when(i == (2 if OFF % 2 else 3))
            def _():
                norm(n)
                tables(n)

            if n < 3:
                slice_in(n + 1, t, slot)
            attention(((0, 1), (2,), (), (3,))[n], t, 1)
            if n == 3:
                @pl.when(t == 6)
                def _():
                    wait_load(woa, ld.at[0, 3])
                    for b in range(4):
                        acc[rows(b), :] = out_attention(b, 0, woa)

                @pl.when(t == LAST - 1)
                def _():
                    here(3 * LAST)
                    load_out(3 * LAST, woa, ld.at[0, 3])

        @pl.when(i == 2)
        def _():
            pltpu.make_async_copy(Pv.at[pl.ds(3, NU - 3)], Pv.at[pl.ds(3, NU - 3)], pack_sem.at[1]).wait()
            own.start()

        @pl.when(i == 4)
        def _():
            own.wait()

        @pl.when((i > 0) & (i < R))
        def _():
            send_own(i)

        for hop in (2, 3, 4):
            s = i - LAG * (hop - 1)

            @pl.when((s >= 0) & (s < R))
            def _():
                cw(s, hop - 1).wait_recv()
                cw(s, hop).start()
                pass_on(s, 9 - hop)
                ccw(s, hop - 1).wait_recv()
                ccw(s, hop).start()
                pass_on(s, hop - 1)

            work(hop - 2)

        s = i - LAG * 4

        @pl.when((s >= 0) & (s < R))
        def _():
            cw(s, 4).wait_recv()
            ccw(s, 4).wait_recv()
            pass_on(s, 4)

        s = i - LAG * 4 - XLAG

        @pl.when((s >= 0) & (s < 2 * M) & (s % 2 == 0))
        def _():
            u = 3 * (s // 2) + 1 - pod
            cross(s // 2, u, 1, 7).wait_recv()
            share(u, c).start()

        work(3)
        s = i - DONE

        @pl.when((s >= 0) & (s < R))
        def _():
            sent(s)

    def sent(s):
        for hop in (1, 2, 3, 4):
            cw(s, hop).wait_send()
            ccw(s, hop).wait_send()
        share(unit_of(s, pod), c).wait_send()

        @pl.when((s < 2 * M) & (s % 2 == 0))
        def _():
            m = s // 2
            cross(m, 3 * m + pod, 1, 7).wait_send()
            share(3 * m + 1 - pod, c).wait_send()

    def two_steps(it, _):
        step(2 * it, 0)
        step(2 * it + 1, 1)
        return 0

    lax.fori_loop(0, STEPS // 2, two_steps, 0)

    last = LAST % 2
    wait_load(wo.at[last], ld.at[last, 2])
    for b in range(4):
        if b == 2:
            here(3 * LAST + 2)
            load_out(3 * LAST + 2, wo.at[1 - last], ld.at[1 - last, 2])
        acc[rows(b), :] = out_attention(b, 2, wo.at[last])
    wait_load(wo.at[1 - last], ld.at[1 - last, 2])
    for b in range(4):
        xv[rows(b), :] = out_attention(b, 3, wo.at[1 - last]).astype(jnp.bfloat16)
        if b:
            y_copy(b - 1).start()
    y_copy(3).start()

    def sent_late(s, _):
        sent(s)
        return 0

    lax.fori_loop(STEPS - DONE, R, sent_late, 0)
    for t in range(1, 16):
        ln_copy(t).wait_send()
    for b in range(4):
        y_copy(b).wait()
    k_copy.wait()
    v_copy.wait()


def layer(x, plen, ln, w_in, w_out, tab):
    bf, f32 = jnp.bfloat16, jnp.float32
    anyspace = pl.BlockSpec(memory_space=pl.ANY)
    vmem = pltpu.VMEM
    dma = pltpu.SemaphoreType.DMA
    return pl.pallas_call(
        layer_kernel,
        name="layer",
        out_shape=(jax.ShapeDtypeStruct((T, E), bf), jax.ShapeDtypeStruct((T, HEAD), bf),
                   jax.ShapeDtypeStruct((T, HEAD), bf), jax.ShapeDtypeStruct((NU, 2, 8, UNIT, 128), bf)),
        in_specs=[anyspace, pl.BlockSpec(memory_space=pltpu.SMEM), pl.BlockSpec(memory_space=vmem),
                  anyspace, anyspace, anyspace],
        out_specs=(anyspace,) * 4,
        scratch_shapes=[
            vmem((NU, UNIT, 128), bf), vmem((T, E), bf), vmem((T, E), bf), vmem((T, E), f32),
            vmem((2, 2, 8, 128, UNIT), bf), vmem((2, 2, 8, 128, UNIT), bf), vmem((2, 8, 128, UNIT), bf),
            vmem((2, UNIT, E), bf), vmem((UNIT, E), bf), vmem((T, UNIT), bf),
            vmem((HEADS, T, HEAD), bf), vmem((T, HEAD), bf), vmem((T, HEAD), bf), vmem((T, HEADS * HEAD), bf),
            vmem((T, 128), f32), vmem((T, 128), f32), vmem((4, 32, 128), f32), vmem((16, 1, 128), f32),
            dma((2,)), dma, dma((2,)), dma((6,)), dma((2, 4)), dma((R, 8)), dma((R, 8)), dma((M,)), dma((M,)),
            dma((NU,)), dma((NU,)), dma((16,)), dma((16,))],
        compiler_params=pltpu.CompilerParams(collective_id=0, has_side_effects=True,
                                             vmem_limit_bytes=63 * 1024 * 1024),
    )(x, plen, ln, w_in, w_out, tab)


def rope_tables():
    freq = ROPE_BASE ** (-2.0 * np.arange(HEAD // 2) / HEAD)
    fine = np.arange(32)[:, None] * freq[None, :]
    return np.stack([np.cos(32 * fine), np.sin(32 * fine), np.cos(fine), np.sin(fine)]).astype(np.float32)


def solution(mesh):
    batch = P(("pod", "d"))
    tab = rope_tables()

    def local_layer(x, plen, ln, w_in, w_out):
        y, k, v, _ = layer(x[0], plen, ln[None], w_in, w_out, tab)
        return y[None], k[None], v[None]

    return jax.shard_map(local_layer, mesh=mesh,
                         in_specs=(batch, batch, P("d"), P("d", None), P(None, "d")),
                         out_specs=(batch, batch, batch), check_vma=False)
```

```python
import functools
import math

import jax
import jax.numpy as jnp
import numpy as np
from jax import lax
from jax.experimental import pallas as pl
from jax.experimental.pallas import tpu as pltpu
from jax.sharding import PartitionSpec as P

MESH = pl.DeviceIdType.MESH
EPS = 1e-6
ROPE_BASE = 10000.0
E, F, HEADS, HEAD, T = 2048, 8192, 8, 256, 1024
Q0, K0 = 2 * F, 2 * F + HEADS * HEAD
UNIT = 512
TRIPLES = 19
NU = 3 * TRIPLES
LAST = TRIPLES - 1
M = 19
R = NU - M
LAG = 1
OFF = 4 * LAG + 1
STEPS = 2 * LAST + OFF + 1
DONE = 8
RB = 256


def unit_of(s, pod):
    m, b = s // 2, s % 2
    return jnp.where(s < 2 * M, 3 * m + (1 - b) * pod + 2 * b, 3 * M + (s - 2 * M))


def device_of(r, c):
    y = r // 4
    z = (1 - y) * r + y * (7 - r)
    return (z * 2 + y) * 2 + c


def layer_kernel(x, plen, ln, w_in, w_out, tab, acc_out, o_out, k_out, v_out, G,
                 Pv, xv, h, acc, wg, wp, wx, wo, woa, a, u1, q, kk, vv, o, cs, sn, tb, ln_all,
                 pack_sem, own_sem, in_sem, out_sem, ld, rs, rr, xs, xr, ds_, dr, ls, lr):
    pod, d = lax.axis_index("pod"), lax.axis_index("d")
    c, yy, zz = d % 2, (d // 2) % 2, d // 4
    r = (1 - yy) * zz + yy * (7 - zz)
    right, left, partner = device_of((r + 1) % 8, c), device_of((r + 7) % 8, c), device_of(r, 1 - c)

    def pack_in(u, col, first=1):
        for j in range(4):
            pltpu.make_async_copy(w_in.at[:, pl.ds(pl.multiple_of(col + 128 * j, 128), 128)],
                                  Pv.at[u, pl.ds(128 * j, 128), :], pack_sem.at[first]).start()

    def pack_out(u, row):
        pltpu.make_async_copy(w_out.at[pl.ds(row, UNIT), :], Pv.at[u], pack_sem.at[1]).start()

    for u, col in ((0, K0), (1, Q0), (2, Q0 + 512)):
        pack_in(u, col, 0)
    bar = pltpu.get_barrier_semaphore()
    for t in range(1, 16):
        pl.semaphore_signal(bar, inc=1, device_id=(pod, (d + t) % 16), device_id_type=MESH)
    pl.semaphore_signal(bar, inc=1, device_id=(1 - pod, d), device_id_type=MESH)
    x_in = pltpu.make_async_copy(x, xv, in_sem.at[0])
    tab_in = pltpu.make_async_copy(tab, tb, in_sem.at[1])
    own = pltpu.make_async_copy(Pv, G.at[:, c, 0], own_sem)
    pltpu.make_async_copy(Pv.at[pl.ds(0, 3)], Pv.at[pl.ds(0, 3)], pack_sem.at[0]).wait()
    pl.semaphore_wait(bar, 16)

    def ring(src, dst, s, e, to):
        return pltpu.make_async_remote_copy(src_ref=src, dst_ref=dst, send_sem=rs.at[s, e], recv_sem=rr.at[s, e],
                                            device_id=(pod, to), device_id_type=MESH)

    half0, half1 = pl.ds(0, 256), pl.ds(256, 256)

    def cw(s, hop):
        u = unit_of(s, pod)
        if hop == 1:
            return ring(Pv.at[u], G.at[u, c, 7], s, 0, right)
        if hop == 4:
            return ring(G.at[u, c, 5, half0], G.at[u, c, 4, half0], s, 6, right)
        return ring(G.at[u, c, 9 - hop], G.at[u, c, 8 - hop], s, 2 * (hop - 1), right)

    def ccw(s, hop):
        u = unit_of(s, pod)
        if hop == 1:
            return ring(Pv.at[u], G.at[u, c, 1], s, 1, left)
        if hop == 4:
            return ring(G.at[u, c, 3, half1], G.at[u, c, 4, half1], s, 7, left)
        return ring(G.at[u, c, hop - 1], G.at[u, c, hop], s, 2 * hop - 1, left)

    def cross(m, u, at, n):
        return pltpu.make_async_remote_copy(src_ref=G.at[u, c, pl.ds(at, n)], dst_ref=G.at[u, c, pl.ds(at, n)],
                                            send_sem=xs.at[m], recv_sem=xr.at[m],
                                            device_id=(1 - pod, d), device_id_type=MESH)

    def share(u, core, at=0, n=8, src=None):
        here = G.at[u, core, pl.ds(at, n)]
        return pltpu.make_async_remote_copy(src_ref=here if src is None else src, dst_ref=here,
                                            send_sem=ds_.at[u], recv_sem=dr.at[u],
                                            device_id=(pod, partner), device_id_type=MESH)

    def pass_on(s, at):
        u = unit_of(s, pod)

        @pl.when((s < 2 * M) & (s % 2 == 0))
        def _():
            cross(s // 2, u, at, 1).start()

        share(u, c, at, 1).start()

    def ln_copy(t):
        return pltpu.make_async_remote_copy(src_ref=ln, dst_ref=ln_all.at[d], send_sem=ls.at[t], recv_sem=lr.at[t],
                                            device_id=(pod, (d + t) % 16), device_id_type=MESH)

    def crossed(m):
        u = 3 * m + 1 - pod
        cross(m, u, 1, 7).wait_recv()
        share(u, c).start()

    def send_own(s):
        cw(s, 1).start()
        ccw(s, 1).start()
        u = unit_of(s, pod)
        share(u, c, 0, 1, Pv.at[pl.ds(u, 1)]).start()

    send_own(0)
    for t in range(1, 16):
        ln_copy(t).start()
    ln_all[pl.ds(d, 1)] = ln[...][None]
    x_in.start()
    tab_in.start()
    for u, col in ((3, Q0 + 1024), (4, Q0 + 1536)):
        pack_in(u, col)
    pack_out(5, F)
    for i in range(3):
        pack_out(3 * LAST + i, F + UNIT * (i + 1))

    def pack_mlp(j, _):
        pack_in(6 + 3 * j, UNIT * j)
        pack_in(7 + 3 * j, F + UNIT * j)
        pack_out(8 + 3 * j, UNIT * j)
        return 0

    lax.fori_loop(0, F // UNIT, pack_mlp, 0)

    def load_in(u, dst, sem):
        for j in range(4):
            pltpu.make_async_copy(G.at[u, :, :, pl.ds(128 * j, 128), :], dst.at[:, :, :, pl.ds(128 * j, 128)], sem).start()

    def load_out(u, dst, sem):
        for cc in range(2):
            for rel in range(8):
                src = device_of((r + rel) % 8, cc)
                pltpu.make_async_copy(G.at[u, cc, rel], dst.at[:, pl.ds(pl.multiple_of(src * 128, 128), 128)], sem).start()

    def wait_load(dst, sem):
        pltpu.make_async_copy(dst, dst, sem).wait()

    def rows(b):
        return pl.ds(b * RB, RB)

    def norm(b):
        xf = xv[rows(b), :].astype(jnp.float32)
        xc = xf - jnp.mean(xf, axis=-1, keepdims=True)
        xn = xc * lax.rsqrt(jnp.mean(xc * xc, axis=-1, keepdims=True) + EPS)
        for src in range(16):
            sc, sy, sz = src % 2, (src // 2) % 2, src // 4
            sr = (1 - sy) * sz + sy * (7 - sz)
            at = sc * 8 + (sr - r + 8) % 8
            h[rows(b), pl.ds(pl.multiple_of(at * 128, 128), 128)] = (
                xn[:, src * 128:(src + 1) * 128] * ln_all[src]).astype(jnp.bfloat16)
        acc[rows(b), :] = xf

    def tables(b):
        cb, sb = tb[2], tb[3]
        for i in range(RB // 32):
            n = b * (RB // 32) + i
            ca, sa = tb[0, n:n + 1, :], tb[1, n:n + 1, :]
            cs[pl.ds(32 * n, 32), :] = ca * cb - sa * sb
            sn[pl.ds(32 * n, 32), :] = sa * cb + ca * sb

    def proj(b, w):
        return jnp.dot(h[rows(b), :], w.reshape(E, UNIT), preferred_element_type=jnp.float32)

    def rope(b, u):
        lo, hi = u[:, :128], u[:, 128:]
        cb, sb = cs[rows(b), :], sn[rows(b), :]
        return jnp.concatenate([lo * cb - hi * sb, hi * cb + lo * sb], axis=-1).astype(jnp.bfloat16)

    def proj_kv(b, w):
        u = proj(b, w)
        kk[rows(b), :] = rope(b, u[:, :256])
        vv[rows(b), :] = u[:, 256:].astype(jnp.bfloat16)

    def proj_q(b, w, head):
        u = proj(b, w)
        q[head, rows(b), :] = rope(b, u[:, :256])
        q[head + 1, rows(b), :] = rope(b, u[:, 256:])

    def attend(b, head):
        n = (b + 1) * RB
        qpos = b * RB + lax.broadcasted_iota(jnp.int32, (RB, n), 0)
        kpos = lax.broadcasted_iota(jnp.int32, (RB, n), 1)
        allowed = (kpos <= qpos) & (kpos < plen[0])

        s = lax.dot_general(q[head, rows(b), :], kk[0:n, :], (((1,), (1,)), ((), ())),
                            preferred_element_type=jnp.float32) * (1.0 / math.sqrt(HEAD))
        s = jnp.where(allowed, s, -1e30)
        e = jnp.exp(s - jnp.max(s, axis=-1, keepdims=True))
        p = (e * (1.0 / jnp.sum(e, axis=-1, keepdims=True))).astype(jnp.bfloat16)
        o[rows(b), pl.ds(pl.multiple_of(head * HEAD, HEAD), HEAD)] = jnp.dot(
            p, vv[0:n, :], preferred_element_type=jnp.float32).astype(jnp.bfloat16)

    def mlp_in(b, slot):
        mine, other = u1[rows(b), :], proj(b, wp[slot])
        g, p = jnp.where(pod == 0, mine, other), jnp.where(pod == 0, other, mine)
        a[rows(b), :] = (g * jax.nn.sigmoid(g) * p).astype(jnp.bfloat16)

    def acc_copy(b):
        return pltpu.make_async_copy(acc.at[rows(b), :], acc_out.at[rows(b), :], out_sem.at[b])

    o_copy = pltpu.make_async_copy(o, o_out, out_sem.at[6])

    k_copy = pltpu.make_async_copy(kk, k_out, out_sem.at[4])
    v_copy = pltpu.make_async_copy(vv, v_out, out_sem.at[5])

    def slice_in(b, t, slot):
        @pl.when(t == 0)
        def _():
            if b == 0:
                wait_load(wg.at[0], ld.at[0, 0])
                wait_load(wp.at[0], ld.at[0, 1])
            proj_kv(b, wg[0])
            proj_q(b, wp[0], 0)

        @pl.when(t == 1)
        def _():
            if b == 0:
                wait_load(wg.at[1], ld.at[1, 0])
            proj_q(b, wg[1], 4)

        @pl.when((t >= 2) & (t < LAST))
        def _():
            if b == 0:
                wait_load(wp.at[slot], ld.at[slot, 1])
            mlp_in(b, slot)

    def slice_out(b, t, slot):
        @pl.when(t == 0)
        def _():
            if b == 0:
                wait_load(wx, ld.at[1, 3])
            proj_q(b, wx[...], 2)

        @pl.when(t == 1)
        def _():
            if b == 0:
                wait_load(wp.at[1], ld.at[1, 1])
            proj_q(b, wp[1], 6)

        @pl.when((t >= 2) & (t < LAST))
        def _():
            if b == 0:
                wait_load(wo.at[slot], ld.at[slot, 2])
            acc[rows(b), :] += jnp.dot(a[rows(b), :], wo[slot], preferred_element_type=jnp.float32)

    def out_attention(b, i, w):
        return acc[rows(b), :] + jnp.dot(o[rows(b), pl.ds(pl.multiple_of(i * UNIT, UNIT), UNIT)], w[...],
                                        preferred_element_type=jnp.float32)

    def attention(blocks, t, second):
        @pl.when((t >= 2) & (t < 2 + HEADS // 2))
        def _():
            for b in blocks:
                attend(b, 2 * (t - 2) + second)

    def here(u):
        share(u, 1 - c).wait_recv()

    def arrive(t):
        slot = t % 2

        @pl.when((t >= 0) & (t < LAST))
        def _():
            @pl.when(t < 2)
            def _():
                here(3 * t + pod)

            here(3 * t + 1 - pod)
            here(3 * t + 2)

        @pl.when(t == 0)
        def _():
            load_in(0, wg.at[0], ld.at[0, 0])
            load_in(1, wp.at[0], ld.at[0, 1])
            load_in(2, wx, ld.at[1, 3])

        @pl.when(t == 1)
        def _():
            load_in(3, wg.at[1], ld.at[1, 0])
            load_in(4, wp.at[1], ld.at[1, 1])

        @pl.when((t >= 2) & (t < LAST))
        def _():
            load_in(3 * t + 1 - pod, wp.at[slot], ld.at[slot, 1])
            load_out(3 * t + 2, wo.at[slot], ld.at[slot, 2])

        @pl.when(t == 6)
        def _():
            load_out(5, woa, ld.at[0, 3])

    def step(i, odd):
        is_out = odd == OFF % 2
        t = jnp.where(i < OFF, -1, (i - OFF) // 2)
        slot = t % 2

        def work(n):
            if is_out:
                before = jnp.where(i < OFF, -1, t - 1)

                @pl.when((t >= 2) & (t < LAST))
                def _():
                    if n == 0:
                        here(3 * t + pod)
                        load_in(3 * t + pod, wg.at[slot], ld.at[slot, 0])
                    if n == 2:
                        wait_load(wg.at[slot], ld.at[slot, 0])
                    if n > 1:
                        for b in (2 * n - 4, 2 * n - 3):
                            u1[rows(b), :] = proj(b, wg[slot])

                if n < 2:
                    slice_out(2 * n, before, (t + 1) % 2)
                    slice_out(2 * n + 1, before, (t + 1) % 2)
                    if n == 1:
                        @pl.when((t >= 0) & (t < LAST))
                        def _():
                            crossed(t)
                elif n == 2:
                    attention((0, 1, 2), t - 1, 1)

                    @pl.when(t == LAST)
                    def _():
                        wait_load(woa, ld.at[0, 3])
                        for b in range(4):
                            acc[rows(b), :] = out_attention(b, 1 + pod, woa)
                            if b:
                                acc_copy(b - 1).start()
                else:
                    attention((3,), t - 1, 1)
                    arrive(t)
                return
            if n == 0:
                @pl.when(i == 2)
                def _():
                    x_in.wait()
                    for j in range(1, 16):
                        ln_copy(j).wait_recv()
                    tab_in.wait()

                @pl.when(t == 2)
                def _():
                    k_copy.start()
                    v_copy.start()

                @pl.when(t == 7)
                def _():
                    o_copy.start()

            @pl.when(i == 2)
            def _():
                norm(n)
                tables(n)

            slice_in(n, t, slot)
            attention((n,), t, 0)
            if n == 3:
                @pl.when(t == 6)
                def _():
                    wait_load(woa, ld.at[0, 3])
                    for b in range(4):
                        acc[rows(b), :] = out_attention(b, 0, woa)

                @pl.when(t == LAST - 1)
                def _():
                    here(3 * LAST + pod)
                    load_out(3 * LAST + pod, woa, ld.at[0, 3])

        @pl.when(i == 2)
        def _():
            pltpu.make_async_copy(Pv.at[pl.ds(3, NU - 3)], Pv.at[pl.ds(3, NU - 3)], pack_sem.at[1]).wait()
            own.start()

        @pl.when(i == 4)
        def _():
            own.wait()

        @pl.when((i > 0) & (i < R))
        def _():
            send_own(i)

        for hop in (2, 3, 4):
            s = i - LAG * (hop - 1)

            @pl.when((s >= 0) & (s < R))
            def _():
                cw(s, hop - 1).wait_recv()
                cw(s, hop).start()
                pass_on(s, 9 - hop)
                ccw(s, hop - 1).wait_recv()
                ccw(s, hop).start()
                pass_on(s, hop - 1)

            work(hop - 2)

        s = i - LAG * 4

        @pl.when((s >= 0) & (s < R))
        def _():
            cw(s, 4).wait_recv()
            ccw(s, 4).wait_recv()
            pass_on(s, 4)

        work(3)
        s = i - DONE

        @pl.when((s >= 0) & (s < R))
        def _():
            sent(s)

    def sent(s):
        for hop in (1, 2, 3, 4):
            cw(s, hop).wait_send()
            ccw(s, hop).wait_send()
        share(unit_of(s, pod), c).wait_send()

        @pl.when((s < 2 * M) & (s % 2 == 0))
        def _():
            m = s // 2
            cross(m, 3 * m + pod, 1, 7).wait_send()
            share(3 * m + 1 - pod, c).wait_send()

    def two_steps(it, _):
        step(2 * it, 0)
        step(2 * it + 1, 1)
        return 0

    lax.fori_loop(0, STEPS // 2, two_steps, 0)

    acc_copy(3).start()
    crossed(LAST)
    here(3 * LAST + 2)
    here(3 * LAST + 1 - pod)

    def sent_late(s, _):
        sent(s)
        return 0

    lax.fori_loop(STEPS - DONE, R, sent_late, 0)
    for t in range(1, 16):
        ln_copy(t).wait_send()
    for b in range(4):
        acc_copy(b).wait()
    k_copy.wait()
    v_copy.wait()
    o_copy.wait()


def finish_kernel(acc, o, k, v, G, y, k_out, v_out, av, ov, wv, yv, kk, vv, in_sem, acc_sem, out_sem):
    pod, d = lax.axis_index("pod"), lax.axis_index("d")
    yy, zz = (d // 2) % 2, d // 4
    r = (1 - yy) * zz + yy * (7 - zz)
    for at, u in ((0, 3 * LAST + 1 - pod), (UNIT, 3 * LAST + 2)):
        for cc in range(2):
            for rel in range(8):
                src = device_of((r + rel) % 8, cc)
                pltpu.make_async_copy(G.at[u, cc, rel],
                                      wv.at[pl.ds(at, UNIT), pl.ds(pl.multiple_of(src * 128, 128), 128)],
                                      in_sem.at[0]).start()
    for at, i in ((0, 2 - pod), (UNIT, 3)):
        pltpu.make_async_copy(o.at[:, pl.ds(pl.multiple_of(i * UNIT, UNIT), UNIT)],
                              ov.at[:, pl.ds(at, UNIT)], in_sem.at[1]).start()
    k_in = pltpu.make_async_copy(k, kk, in_sem.at[2])
    v_in = pltpu.make_async_copy(v, vv, in_sem.at[3])
    k_copy = pltpu.make_async_copy(kk, k_out, out_sem.at[4])
    v_copy = pltpu.make_async_copy(vv, v_out, out_sem.at[5])

    def rows(b):
        return pl.ds(b * RB, RB)

    def acc_in(b):
        return pltpu.make_async_copy(acc.at[rows(b), :], av.at[rows(b), :], acc_sem.at[b])

    def y_copy(b):
        return pltpu.make_async_copy(yv.at[rows(b), :], y.at[rows(b), :], out_sem.at[b])

    acc_in(0).start()
    pltpu.make_async_copy(wv, wv, in_sem.at[0]).wait()
    for b in range(1, 4):
        acc_in(b).start()
    k_in.start()
    v_in.start()
    pltpu.make_async_copy(ov, ov, in_sem.at[1]).wait()
    for b in range(4):
        acc_in(b).wait()
        if b == 3:
            k_in.wait()
            v_in.wait()
            k_copy.start()
            v_copy.start()
        yv[rows(b), :] = (av[rows(b), :] + jnp.dot(ov[rows(b), :], wv[...], preferred_element_type=jnp.float32)
                          ).astype(jnp.bfloat16)
        if b:
            y_copy(b - 1).start()
    y_copy(3).start()
    for b in range(4):
        y_copy(b).wait()
    k_copy.wait()
    v_copy.wait()


def layer(x, plen, ln, w_in, w_out, tab):
    bf, f32 = jnp.bfloat16, jnp.float32
    anyspace = pl.BlockSpec(memory_space=pl.ANY)
    vmem = pltpu.VMEM
    dma = pltpu.SemaphoreType.DMA
    acc, o, k, v, gathered = pl.pallas_call(
        layer_kernel,
        name="layer",
        out_shape=(jax.ShapeDtypeStruct((T, E), f32), jax.ShapeDtypeStruct((T, HEADS * HEAD), bf),
                   jax.ShapeDtypeStruct((T, HEAD), bf),
                   jax.ShapeDtypeStruct((T, HEAD), bf), jax.ShapeDtypeStruct((NU, 2, 8, UNIT, 128), bf)),
        in_specs=[anyspace, pl.BlockSpec(memory_space=pltpu.SMEM), pl.BlockSpec(memory_space=vmem),
                  anyspace, anyspace, anyspace],
        out_specs=(anyspace,) * 5,
        scratch_shapes=[
            vmem((NU, UNIT, 128), bf), vmem((T, E), bf), vmem((T, E), bf), vmem((T, E), f32),
            vmem((2, 2, 8, 128, UNIT), bf), vmem((2, 2, 8, 128, UNIT), bf), vmem((2, 8, 128, UNIT), bf),
            vmem((2, UNIT, E), bf), vmem((UNIT, E), bf), vmem((T, UNIT), bf), vmem((T, UNIT), f32),
            vmem((HEADS, T, HEAD), bf), vmem((T, HEAD), bf), vmem((T, HEAD), bf), vmem((T, HEADS * HEAD), bf),
            vmem((T, 128), f32), vmem((T, 128), f32), vmem((4, 32, 128), f32), vmem((16, 1, 128), f32),
            dma((2,)), dma, dma((2,)), dma((7,)), dma((2, 4)), dma((R, 8)), dma((R, 8)), dma((M,)), dma((M,)),
            dma((NU,)), dma((NU,)), dma((16,)), dma((16,))],
        compiler_params=pltpu.CompilerParams(collective_id=0, has_side_effects=True,
                                             vmem_limit_bytes=63 * 1024 * 1024),
    )(x, plen, ln, w_in, w_out, tab)
    return pl.pallas_call(
        finish_kernel,
        name="finish_layer",
        out_shape=(jax.ShapeDtypeStruct((T, E), bf), jax.ShapeDtypeStruct((T, HEAD), bf),
                   jax.ShapeDtypeStruct((T, HEAD), bf)),
        in_specs=[anyspace] * 5,
        out_specs=(anyspace,) * 3,
        scratch_shapes=[vmem((T, E), f32), vmem((T, 2 * UNIT), bf), vmem((2 * UNIT, E), bf), vmem((T, E), bf),
                        vmem((T, HEAD), bf), vmem((T, HEAD), bf), dma((4,)), dma((4,)), dma((6,))],
        compiler_params=pltpu.CompilerParams(vmem_limit_bytes=63 * 1024 * 1024),
    )(acc, o, k, v, gathered)


def rope_tables():
    freq = ROPE_BASE ** (-2.0 * np.arange(HEAD // 2) / HEAD)
    fine = np.arange(32)[:, None] * freq[None, :]
    return np.stack([np.cos(32 * fine), np.sin(32 * fine), np.cos(fine), np.sin(fine)]).astype(np.float32)


def solution(mesh):
    batch = P(("pod", "d"))
    tab = rope_tables()

    def local_layer(x, plen, ln, w_in, w_out):
        y, k, v = layer(x[0], plen, ln[None], w_in, w_out, tab)
        return y[None], k[None], v[None]

    return jax.shard_map(local_layer, mesh=mesh,
                         in_specs=(batch, batch, P("d"), P("d", None), P(None, "d")),
                         out_specs=(batch, batch, batch), check_vma=False)
```
